32 devices in a mesh: ep: 4 (over y, core), fsdp: 8 (over z, x).
Axes of the slice: x: 2, y: 2, z: 4, core: 2. Of those that a mesh axis runs over, the one named last changes fastest.
Arguments:
- w_down: float32 [16, 6400, 4096], P('ep', None, 'fsdp'), may hold values from -0.109375 to 0.109375
- router_weight: float32 [4096, 16], P('fsdp', 'ep'), may hold values from -0.09375 to 0.09375
- router_gain: float32 [4096], P('fsdp'), may hold values from 0.25 to 1.75
Outputs:
- serve_down: bfloat16 [16, 6400, 4096], P('ep', 'fsdp')
- scale_down: float32 [16, 6400], P('ep', 'fsdp')
- serve_router: bfloat16 [4096, 16], replicated
The draws below stay inside these ranges and needn't reach their ends.
All inputs are finite; a program needn't handle non-finite values.
Results may differ from the reference program's by a relative error of at most 0.001.
Values may be sent and summed in bfloat16 or wider, within the bound.
A program may use at most 192 MiB of HBM per device.

```python
import jax
import jax.numpy as jnp
from jax import lax

EXPERTS = 16
D_MODEL = 4096
D_EXPERT = 6400


def strengthened(entries, key, source, target, parts, factor):
    def block_of(axis_at):
        return (jnp.arange(entries.shape[axis_at]) // (entries.shape[axis_at] // parts)).reshape((-1,) + (1,) * (entries.ndim - 1 - axis_at))

    near = jax.random.permutation(key, parts)[block_of(target)]
    second = (block_of(target) + parts // 2) % parts
    return jnp.where((block_of(source) == near) | (block_of(source) == second), factor * entries, entries)


def shard_levels(stream_key, extent, cuts, low, high):
    gain = 1.0
    for position, parts in cuts:
        heights = jax.random.uniform(jax.random.fold_in(jax.random.fold_in(stream_key, 6), position), (parts,), jnp.float32, low / len(cuts), high / len(cuts))
        gain = gain * jnp.repeat(jnp.exp(heights), extent[position] // parts).reshape((-1,) + (1,) * (len(extent) - 1 - position))
    return gain


def scatter_about(rng, extent, width, limit, pieces=(), held_as=jnp.bfloat16):
    entries = width * jax.random.normal(rng, extent, jnp.float32)
    if pieces:
        entries = entries * shard_levels(rng, extent, pieces, -0.22, 0.18)
    return jnp.clip(entries, -limit, limit).astype(held_as)


def heavy_noise(own_key, dims, deviation, limit, shards, heavy, held_as=jnp.bfloat16):
    array = deviation * jax.random.normal(own_key, dims, jnp.float32)
    if shards:
        array = array * shard_levels(own_key, dims, shards, -0.22, 0.18)
    return jnp.clip(strengthened(array, jax.random.fold_in(own_key, 3), *heavy), -limit, limit).astype(held_as)


def setup_inputs(seed: int = 0) -> dict:
    arg_keys = jax.random.split(jax.random.key(seed), 4)
    return {
        "w_down": heavy_noise(arg_keys[0], (EXPERTS, D_EXPERT, D_MODEL), D_EXPERT ** -0.5, 0.109375, ((0, 4), (2, 8)), (2, 1, 8, 2.0), jnp.float32),
        "router_weight": scatter_about(arg_keys[1], (D_MODEL, EXPERTS), D_MODEL ** -0.5, 0.09375, ((0, 8), (1, 4)), jnp.float32),
        "router_gain": jnp.clip(1.0 + 0.15 * jax.random.normal(arg_keys[2], (D_MODEL,), jnp.float32), 0.25, 1.75),
    }


def reference(w_down, router_weight, router_gain):
    scale_down = jnp.sqrt(lax.optimization_barrier(jnp.sum(w_down * w_down, axis=2)))
    serve_down = (w_down / jnp.expand_dims(scale_down, 2)).astype(jnp.bfloat16)
    serve_router = (router_weight * router_gain[:, None]).astype(jnp.bfloat16)
    return (serve_down, scale_down, serve_router)
```

```python
import functools

import jax
import jax.numpy as jnp
from jax import lax
from jax.experimental import pallas as pl
from jax.experimental.pallas import tpu as pltpu
from jax.sharding import PartitionSpec as P

LANES = 128
MESH = pl.DeviceIdType.MESH


def target(me, j, n):
    h = n // 2
    side = me // h
    m = me + side * (n - 1 - 2 * me)
    inner = m // max(n // 4, 1)
    half = j // 2
    odd = j % 2
    d_in = (1 - odd) * (h + (half + m) % h) + odd * ((m + 1 + half) % h)
    far = (j + 1) // h
    d_out = (1 - far) * ((m + 1 + j) % h) + far * (h + (j + 1 - h + m) % h)
    d = inner * d_in + (1 - inner) * d_out
    d = d + side * (n - 1 - 2 * d)
    last = (j + 1) // n
    return last * me + (1 - last) * d


def kernel(n, w, o, sc, xbuf, sbuf, part, recvp, mine, scales,
           load_sem, send_sem, recv_sem, psend, precv, ssend, srecv, own_sem):
    experts, rows, cols = w.shape
    block = rows // n
    tiles = -(-block // LANES)
    padded = part.shape[2]
    starts = [min(t * LANES, block - LANES) for t in range(tiles)]
    steps = n * experts
    slots = xbuf.shape[0]
    me = lax.axis_index("fsdp")

    def where(i):
        return target(me, i // experts, n), i % experts

    def load(i):
        d, e = where(i)
        s = i % slots
        return pltpu.make_async_copy(
            w.at[e, pl.ds(pl.multiple_of(d * block, 8), block), :], xbuf.at[s], load_sem.at[s])

    def peer(j):
        return target(me, j, n)

    def sums(to, source):
        return pltpu.make_async_remote_copy(
            src_ref=part.at[to], dst_ref=recvp.at[source], send_sem=psend.at[to],
            recv_sem=precv.at[source], device_id={"fsdp": to}, device_id_type=MESH)

    def scale_copy(to, source):
        return pltpu.make_async_remote_copy(
            src_ref=mine, dst_ref=scales.at[source], send_sem=ssend.at[to],
            recv_sem=srecv.at[source], device_id={"fsdp": to}, device_id_type=MESH)

    def bulk(i, to, e, source):
        return pltpu.make_async_remote_copy(
            src_ref=sbuf.at[i],
            dst_ref=o.at[e, :, pl.ds(pl.multiple_of(source * cols, LANES), cols)],
            send_sem=send_sem.at[i], recv_sem=recv_sem.at[source * experts + e],
            device_id={"fsdp": to}, device_id_type=MESH)

    def local(i, e):
        return pltpu.make_async_copy(
            sbuf.at[i], o.at[e, :, pl.ds(pl.multiple_of(me * cols, LANES), cols)], own_sem.at[e])

    def each(count, f):
        def step(i, c):
            f(i)
            return c
        lax.fori_loop(0, count, step, 0)

    each(slots, lambda k: load(steps - 1 - k).start())

    barrier = pltpu.get_barrier_semaphore()
    each(n - 1, lambda j: pl.semaphore_signal(
        barrier, inc=1, device_id={"fsdp": peer(j)}, device_id_type=MESH))
    pl.semaphore_wait(barrier, n - 1)

    def first(k):
        i = steps - 1 - k
        d, e = where(i)
        s = i % slots
        load(i).wait()
        found = []
        for start in starts:
            x = xbuf[s, start:start + LANES, :]
            y = x * x
            acc = y[:, :LANES]
            for c in range(LANES, cols, LANES):
                acc = acc + y[:, c:c + LANES]
            found.append(jnp.sum(acc.T, axis=0, keepdims=True))
        if padded > tiles:
            found.append(jnp.zeros((padded - tiles, LANES), jnp.float32))
        part[d, e] = jnp.concatenate(found, axis=0)

        @pl.when(i >= slots)
        def _():
            load(i - slots).start()

        @pl.when((e == 0) & (i // experts < n - 1))
        def _():
            sums(d, me).start()

    each(steps, first)

    def add(j, total):
        source = peer(j)
        sums(source, source).wait_recv()
        return total + recvp[source]

    total = lax.fori_loop(0, n - 1, add, part[me])
    scale = jnp.sqrt(total)
    sc[...] = scale
    mine[...] = scale
    scales[me] = scale
    each(n - 1, lambda j: scale_copy(peer(j), me).start())

    def second(i):
        d, e = where(i)
        s = i % slots

        @pl.when((e == 0) & (i // experts < n - 1))
        def _():
            scale_copy(d, d).wait_recv()

        @pl.when(i >= slots)
        def _():
            load(i).wait()

        inverse = 1.0 / scales[d, e]
        for t, start in enumerate(starts):
            factor = jnp.broadcast_to(inverse[t:t + 1, :], (LANES, LANES)).T
            for c in range(0, cols, LANES):
                x = xbuf[s, start:start + LANES, c:c + LANES]
                sbuf[i, start:start + LANES, c:c + LANES] = (x * factor).astype(jnp.bfloat16)

        @pl.when(i + slots < steps)
        def _():
            load(i + slots).start()

        @pl.when(i // experts < n - 1)
        def _():
            bulk(i, d, e, me).start()

        @pl.when(i // experts == n - 1)
        def _():
            local(i, e).start()

    each(steps, second)

    def drain(i):
        d, e = where(i)
        bulk(i, d, e, me).wait_send()
        bulk(i, d, e, d).wait_recv()

    def finish(j):
        sums(peer(j), me).wait_send()
        scale_copy(peer(j), me).wait_send()

    each(n - 1, finish)
    each(experts, lambda e: local(steps - experts + e, e).wait())
    each(steps - experts, drain)


def exchange(n, w):
    experts, rows, cols = w.shape
    block = rows // n
    tiles = -(-block // LANES)
    padded = -(-tiles // 8) * 8
    steps = n * experts
    slots = min(2 * n, steps)
    sums = (n, experts, padded, LANES)
    dma = pltpu.SemaphoreType.DMA
    o, sc = pl.pallas_call(
        functools.partial(kernel, n),
        out_shape=(
            jax.ShapeDtypeStruct((experts, block, n * cols), jnp.bfloat16),
            jax.ShapeDtypeStruct((experts, padded, LANES), jnp.float32),
        ),
        in_specs=[pl.BlockSpec(memory_space=pl.ANY)],
        out_specs=(pl.BlockSpec(memory_space=pl.ANY), pl.BlockSpec(memory_space=pltpu.VMEM)),
        scratch_shapes=[
            pltpu.VMEM((slots, block, cols), jnp.float32),
            pltpu.VMEM((steps, block, cols), jnp.bfloat16),
            pltpu.VMEM(sums, jnp.float32),
            pltpu.VMEM(sums, jnp.float32),
            pltpu.VMEM(sums[1:], jnp.float32),
            pltpu.VMEM(sums, jnp.float32),
            dma((slots,)), dma((steps,)), dma((steps,)),
            dma((n,)), dma((n,)), dma((n,)), dma((n,)), dma((experts,)),
        ],
        compiler_params=pltpu.CompilerParams(
            collective_id=0, has_side_effects=True, vmem_limit_bytes=58 * 1024 * 1024),
    )(w)
    tail = block - (tiles - 1) * LANES
    scale = jnp.concatenate(
        [sc[:, :tiles - 1].reshape(experts, (tiles - 1) * LANES), sc[:, tiles - 1, LANES - tail:]], axis=1)
    return o, scale


def body(n, w_down, router_weight, router_gain):
    serve_down, scale_down = exchange(n, w_down)
    part_router = (router_weight * router_gain[:, None]).astype(jnp.bfloat16)
    row_router = lax.all_gather(part_router, "fsdp", axis=0, tiled=True)
    serve_router = lax.all_gather(row_router, "ep", axis=1, tiled=True)
    return (serve_down, scale_down, serve_router)


def solution(mesh):
    in_specs = (P("ep", None, "fsdp"), P("fsdp", "ep"), P("fsdp"))
    out_specs = (P("ep", "fsdp", None), P("ep", "fsdp"), P())
    return jax.shard_map(
        functools.partial(body, mesh.shape["fsdp"]), mesh=mesh,
        in_specs=in_specs, out_specs=out_specs, check_vma=False)
```

```python
import functools

import jax
import jax.numpy as jnp
from jax import lax
from jax.experimental import pallas as pl
from jax.experimental.pallas import tpu as pltpu
from jax.sharding import PartitionSpec as P

LANES = 128
MESH = pl.DeviceIdType.MESH


def target(me, j, n):
    return (me + j + 1) % n


def kernel(n, w, o, sc, xbuf, sbuf, part, recvp, mine, scales,
           load_sem, send_sem, recv_sem, psend, precv, ssend, srecv, own_sem):
    experts, rows, cols = w.shape
    block = rows // n
    tiles = -(-block // LANES)
    padded = part.shape[2]
    starts = [min(t * LANES, block - LANES) for t in range(tiles)]
    steps = n * experts
    slots = xbuf.shape[0]
    me = lax.axis_index("fsdp")

    def where(i):
        return target(me, i // experts, n), i % experts

    def load(i):
        d, e = where(i)
        s = i % slots
        return pltpu.make_async_copy(
            w.at[e, pl.ds(pl.multiple_of(d * block, 8), block), :], xbuf.at[s], load_sem.at[s])

    def peer(j):
        return target(me, j, n)

    def sums(to, source):
        return pltpu.make_async_remote_copy(
            src_ref=part.at[to], dst_ref=recvp.at[source], send_sem=psend.at[to],
            recv_sem=precv.at[source], device_id={"fsdp": to}, device_id_type=MESH)

    def scale_copy(to, source):
        return pltpu.make_async_remote_copy(
            src_ref=mine, dst_ref=scales.at[source], send_sem=ssend.at[to],
            recv_sem=srecv.at[source], device_id={"fsdp": to}, device_id_type=MESH)

    def bulk(i, to, e, source):
        return pltpu.make_async_remote_copy(
            src_ref=sbuf.at[i],
            dst_ref=o.at[e, :, pl.ds(pl.multiple_of(source * cols, LANES), cols)],
            send_sem=send_sem.at[i], recv_sem=recv_sem.at[source * experts + e],
            device_id={"fsdp": to}, device_id_type=MESH)

    def local(i, e):
        return pltpu.make_async_copy(
            sbuf.at[i], o.at[e, :, pl.ds(pl.multiple_of(me * cols, LANES), cols)], own_sem.at[e])

    def each(count, f):
        def step(i, c):
            f(i)
            return c
        lax.fori_loop(0, count, step, 0)

    each(slots, lambda k: load(steps - 1 - k).start())

    barrier = pltpu.get_barrier_semaphore()
    each(n - 1, lambda j: pl.semaphore_signal(
        barrier, inc=1, device_id={"fsdp": peer(j)}, device_id_type=MESH))
    pl.semaphore_wait(barrier, n - 1)

    def first(k):
        i = steps - 1 - k
        d, e = where(i)
        s = i % slots
        load(i).wait()
        found = []
        for start in starts:
            x = xbuf[s, start:start + LANES, :]
            y = x * x
            acc = y[:, :LANES]
            for c in range(LANES, cols, LANES):
                acc = acc + y[:, c:c + LANES]
            found.append(jnp.sum(acc.T, axis=0, keepdims=True))
        if padded > tiles:
            found.append(jnp.zeros((padded - tiles, LANES), jnp.float32))
        part[d, e] = jnp.concatenate(found, axis=0)

        @pl.when(i >= slots)
        def _():
            load(i - slots).start()

        @pl.when((e == 0) & (i // experts < n - 1))
        def _():
            sums(d, me).start()

    each(steps, first)

    def add(j, total):
        source = peer(j)
        sums(source, source).wait_recv()
        return total + recvp[source]

    total = lax.fori_loop(0, n - 1, add, part[me])
    scale = jnp.sqrt(total)
    sc[...] = scale
    mine[...] = scale
    scales[me] = scale
    each(n - 1, lambda j: scale_copy(peer(j), me).start())

    def second(i):
        d, e = where(i)
        s = i % slots

        @pl.when((e == 0) & (i // experts < n - 1))
        def _():
            scale_copy(d, d).wait_recv()

        @pl.when(i >= slots)
        def _():
            load(i).wait()

        inverse = 1.0 / scales[d, e]
        for t, start in enumerate(starts):
            factor = jnp.broadcast_to(inverse[t:t + 1, :], (LANES, LANES)).T
            for c in range(0, cols, LANES):
                x = xbuf[s, start:start + LANES, c:c + LANES]
                sbuf[i, start:start + LANES, c:c + LANES] = (x * factor).astype(jnp.bfloat16)

        @pl.when(i + slots < steps)
        def _():
            load(i + slots).start()

        @pl.when(i // experts < n - 1)
        def _():
            bulk(i, d, e, me).start()

        @pl.when(i // experts == n - 1)
        def _():
            local(i, e).start()

    each(steps, second)

    def drain(i):
        d, e = where(i)
        bulk(i, d, e, me).wait_send()
        bulk(i, d, e, d).wait_recv()

    def finish(j):
        sums(peer(j), me).wait_send()
        scale_copy(peer(j), me).wait_send()

    each(n - 1, finish)
    each(experts, lambda e: local(steps - experts + e, e).wait())
    each(steps - experts, drain)


def exchange(n, w):
    experts, rows, cols = w.shape
    block = rows // n
    tiles = -(-block // LANES)
    padded = -(-tiles // 8) * 8
    steps = n * experts
    slots = min(2 * n, steps)
    sums = (n, experts, padded, LANES)
    dma = pltpu.SemaphoreType.DMA
    o, sc = pl.pallas_call(
        functools.partial(kernel, n),
        out_shape=(
            jax.ShapeDtypeStruct((experts, block, n * cols), jnp.bfloat16),
            jax.ShapeDtypeStruct((experts, padded, LANES), jnp.float32),
        ),
        in_specs=[pl.BlockSpec(memory_space=pl.ANY)],
        out_specs=(pl.BlockSpec(memory_space=pl.ANY), pl.BlockSpec(memory_space=pltpu.VMEM)),
        scratch_shapes=[
            pltpu.VMEM((slots, block, cols), jnp.float32),
            pltpu.VMEM((steps, block, cols), jnp.bfloat16),
            pltpu.VMEM(sums, jnp.float32),
            pltpu.VMEM(sums, jnp.float32),
            pltpu.VMEM(sums[1:], jnp.float32),
            pltpu.VMEM(sums, jnp.float32),
            dma((slots,)), dma((steps,)), dma((steps,)),
            dma((n,)), dma((n,)), dma((n,)), dma((n,)), dma((experts,)),
        ],
        compiler_params=pltpu.CompilerParams(
            collective_id=0, has_side_effects=True, vmem_limit_bytes=58 * 1024 * 1024),
    )(w)
    tail = block - (tiles - 1) * LANES
    scale = jnp.concatenate(
        [sc[:, :tiles - 1].reshape(experts, (tiles - 1) * LANES), sc[:, tiles - 1, LANES - tail:]], axis=1)
    return o, scale


def body(n, w_down, router_weight, router_gain):
    serve_down, scale_down = exchange(n, w_down)
    part_router = (router_weight * router_gain[:, None]).astype(jnp.bfloat16)
    row_router = lax.all_gather(part_router, "fsdp", axis=0, tiled=True)
    serve_router = lax.all_gather(row_router, "ep", axis=1, tiled=True)
    return (serve_down, scale_down, serve_router)


def solution(mesh):
    in_specs = (P("ep", None, "fsdp"), P("fsdp", "ep"), P("fsdp"))
    out_specs = (P("ep", "fsdp", None), P("ep", "fsdp"), P())
    return jax.shard_map(
        functools.partial(body, mesh.shape["fsdp"]), mesh=mesh,
        in_specs=in_specs, out_specs=out_specs, check_vma=False)
```
